32 devices in a mesh: hap: 16 (over z, x, core), mk: 2 (over y).
Axes of the slice: x: 2, y: 2, z: 4, core: 2. Of those that a mesh axis runs over, the one named last changes fastest.
Arguments:
- posterior: bfloat16 [10, 1024, 16384], P('mk', None, 'hap'), may hold values from 0 to 1, as said below
- alleles: int32 [16384, 64], P('hap', 'mk'), may hold values from 0 to 1
- owner_map: int32 [1024], replicated, may hold values from 0 to 31, as said below
Outputs:
- dosage: float32 [1024, 64], P(('hap', 'mk'))
The draws below stay inside these ranges and needn't reach their ends.
Inputs may be any that keep to these rules, and one draw needn't show every extreme that they name: `owner_map`: every device index is named by exactly 32 targets. `posterior`: every entry is positive.
All inputs are finite; a program needn't handle non-finite values.
Results may differ from the reference program's by a relative error of at most 0.0003.
Values sent between devices are 32-bit elements; how exact they have to be, the bound alone decides.
A program may use at most 64 MiB of HBM per device.

```python
import jax
import jax.numpy as jnp
from jax import lax

TGT = 1024
ANCH = 5
MB = 32
MARKERS = 64
REF = 16384
TOWN = 32
N_HAP = 16
N_MK = 2


def draw_owner_map(key, part):
    return (jax.random.permutation(key, TGT) // TOWN).astype(jnp.int32)


def draw_alleles(key, part):
    level_key = jax.random.fold_in(key, 11)
    cell_key = jax.random.fold_in(key, 12)
    level = jax.random.randint(level_key, (1, MARKERS), 1, 1024, dtype=jnp.int32)
    cell = jax.random.randint(cell_key, (REF, MARKERS), 0, 1024, dtype=jnp.int32)
    return (cell < level).astype(jnp.int32)


def draw_posterior(key, part):
    chooser = jax.random.uniform(jax.random.fold_in(key, 21), (ANCH * N_MK, TGT, REF), jnp.float32)
    chance = 16.0 / REF
    peak = 0.25 + 0.74 * (chooser / chance)
    floor_low = jnp.log(1e-05)
    floor_high = jnp.log(0.0001)
    rest = jnp.clip((chooser - chance) / (1.0 - chance), 0.0, 1.0)
    floor = jnp.exp(floor_low + rest * (floor_high - floor_low))
    values = jnp.where(chooser < chance, peak, floor)
    return values.astype(jnp.bfloat16)


def setup_inputs(seed: int = 0) -> dict:
    key_list = jax.random.split(jax.random.key(seed), 4)
    posterior = draw_posterior(jax.random.fold_in(key_list[3], 71), 0)
    alleles = draw_alleles(jax.random.fold_in(key_list[3], 71), 0)
    owner_map = draw_owner_map(jax.random.fold_in(key_list[3], 71), 0)
    return {"posterior": posterior, "alleles": alleles, "owner_map": owner_map}


def interpolate(numerator, denominator):
    anchors = numerator.shape[0]
    intervals = anchors - 1
    block_width = numerator.shape[-1]
    marker_span = block_width // intervals
    ratios = numerator / denominator[:, :, None]
    column = jnp.arange(block_width, dtype=jnp.int32)
    interval = column // marker_span
    weight = ((column % marker_span).astype(jnp.float32) + 0.5) / marker_span
    picker = (interval[None, :] == jnp.arange(intervals, dtype=jnp.int32)[:, None]).astype(jnp.float32)
    left_part = jnp.sum(picker[:, None, :] * ratios[:-1], axis=0)
    right_part = jnp.sum(picker[:, None, :] * ratios[1:], axis=0)
    return (1.0 - weight) * left_part + weight * right_part


def positions(owner_map, devices, per_device):
    owner_table = (owner_map[:, None] == jnp.arange(devices, dtype=jnp.int32)[None, :]).astype(jnp.int32)
    owner_rank = jnp.sum(jnp.cumsum(owner_table, axis=0) * owner_table, axis=1) - 1
    return (owner_map * per_device + owner_rank).astype(jnp.int32)


def reference(posterior, alleles, owner_map):
    allele_bf = alleles.astype(jnp.bfloat16)
    unit_vector = jnp.ones((REF,), jnp.bfloat16)

    def one_anchor(index):
        group = (index // ANCH).astype(jnp.int32)
        matrix = lax.dynamic_index_in_dim(posterior, index, 0, keepdims=False)
        columns = lax.dynamic_slice_in_dim(allele_bf, group * MB, MB, 1)
        top = jnp.dot(matrix, columns, preferred_element_type=jnp.float32)
        bottom = jnp.dot(matrix, unit_vector, preferred_element_type=jnp.float32)
        return top, bottom

    numerator, denominator = lax.map(one_anchor, jnp.arange(ANCH * N_MK, dtype=jnp.int32))
    numerator = numerator.reshape(N_MK, ANCH, TGT, MB)
    denominator = denominator.reshape(N_MK, ANCH, TGT)
    block_dose = jax.vmap(interpolate)(numerator, denominator)
    all_markers = jnp.transpose(block_dose, (1, 0, 2)).reshape(TGT, MARKERS)
    row_of = positions(owner_map, N_HAP * N_MK, TOWN)
    return jnp.zeros((TGT, MARKERS), jnp.float32).at[row_of].set(all_markers)
```

```python
import functools

import jax
import jax.numpy as jnp
from jax import lax
from jax.experimental import pallas as pl
from jax.experimental.pallas import tpu as pltpu
from jax.sharding import PartitionSpec as P

LANES = 128
HALF = LANES // 2
CORES = 2
MESH = pl.DeviceIdType.MESH
F32 = jnp.float32
BF16 = jnp.bfloat16


def own_rows(ref, index, count):
    if count % 8 == 0:
        return ref[pl.ds(pl.multiple_of(index * count, 8), count), :]
    pieces = 8 // count
    tile = ref[pl.ds(pl.multiple_of((index // pieces) * 8, 8), 8), :]
    rows = tile[:count]
    for piece in range(1, pieces):
        rows = jnp.where(index % pieces == piece, tile[piece * count : (piece + 1) * count], rows)
    return rows


def kernel(
    hap_count,
    mk_count,
    steps,
    post_hbm,
    allele_hbm,
    owner_hbm,
    out_ref,
    post,
    allele,
    owner,
    weights,
    choose,
    parts,
    mine,
    pair_in,
    reduced,
    chip_in,
    final,
    turned,
    post_sem,
    small_sem,
    pair_send,
    pair_recv,
    chip_send,
    chip_recv,
    final_send,
    final_recv,
):
    anchors, targets, _ = post.shape
    block = allele.shape[0]
    intervals = anchors - 1
    span = block // intervals
    local = intervals // CORES
    body = 2 * local * span
    rows_kept = mine.shape[1] // CORES
    chips = hap_count // CORES
    per_chip = targets // chips
    devices = hap_count * mk_count
    per_device = targets // devices
    group = CORES * mk_count
    chunk = targets // steps

    hap, mk = lax.axis_index("hap"), lax.axis_index("mk")
    chip, core = hap // CORES, hap % CORES
    place = mk * CORES + core

    def chip_peer(step):
        return {"hap": ((chip + step) % chips) * CORES + core, "mk": mk}

    def group_peer(step):
        other = (place + step) % group
        return {"hap": chip * CORES + other % CORES, "mk": other // CORES}

    allele_copy = pltpu.make_async_copy(allele_hbm, allele, small_sem.at[0])
    owner_copy = pltpu.make_async_copy(owner_hbm, owner, small_sem.at[1])
    owner_copy.start()
    allele_copy.start()
    post_copies = []
    for i in range(steps):
        rows = pl.ds(i * chunk, chunk)
        copy = pltpu.make_async_copy(post_hbm.at[:, rows, :], post.at[:, rows, :], post_sem.at[i])
        copy.start()
        post_copies.append(copy)

    barrier = pltpu.get_barrier_semaphore()
    for step in range(1, chips):
        pl.semaphore_signal(barrier, inc=1, device_id=chip_peer(step), device_id_type=MESH)
    for step in range(1, group):
        pl.semaphore_signal(barrier, inc=1, device_id=group_peer(step), device_id_type=MESH)

    owner_copy.wait()
    owners = owner[...]
    table = (lax.broadcasted_iota(jnp.int32, (devices, targets), 0) == owners).astype(F32)
    before = (
        lax.broadcasted_iota(jnp.int32, (LANES, LANES), 0)
        < lax.broadcasted_iota(jnp.int32, (LANES, LANES), 1)
    ).astype(F32).astype(BF16)
    carry = jnp.zeros((devices, 1), F32)
    ranks = []
    for b in range(targets // LANES):
        piece = table[:, b * LANES : (b + 1) * LANES]
        count = jnp.dot(piece.astype(BF16), before, preferred_element_type=F32) + carry
        ranks.append(jnp.sum(piece * count, axis=0, keepdims=True))
        carry = carry + jnp.sum(piece, axis=1, keepdims=True)
    row_of = owners.astype(F32) * per_device + jnp.concatenate(ranks, axis=1)

    order = sorted(range(1, chips), key=lambda s: abs(s - chips // 2 - 0.5)) + [0]

    for step in order:
        first = ((chip + step) % chips) * per_chip
        wanted = (lax.broadcasted_iota(jnp.int32, (per_chip, targets), 0) + first).astype(F32)
        choose[step] = (wanted == row_of).astype(F32).astype(BF16)

    allele_copy.wait()
    col = lax.broadcasted_iota(jnp.int32, (block, LANES), 1)
    marker = lax.broadcasted_iota(jnp.int32, (block, LANES), 0)
    lane = lax.broadcasted_iota(jnp.int32, (1, LANES), 1)
    spread = jnp.zeros((block, LANES), F32)
    starts = []
    for j in range(intervals):
        for side in range(2):
            start = (j // local) * HALF + (j % local) * 2 * span + side * span
            starts.append((j + side, start))
            hit = (col - start == marker - j * span) & (col >= start) & (col < start + span)
            spread = spread + hit.astype(F32)
    wide = lax.dot_general(
        allele[...].astype(F32).astype(BF16),
        spread.astype(BF16),
        (((0,), (0,)), ((), ())),
        preferred_element_type=F32,
    )
    for k in range(anchors):
        inside = jnp.zeros((1, LANES), F32)
        for anchor, start in starts:
            if anchor == k:
                inside = inside + ((lane >= start) & (lane < start + span)).astype(F32)
        ones = jnp.zeros((1, LANES), F32)
        for c in range(CORES):
            if c * local <= k <= (c + 1) * local:
                ones = ones + (lane == c * HALF + body + k - c * local).astype(F32)
        weights[k] = (wide * inside + ones).astype(BF16)

    for i in range(steps):
        rows = pl.ds(i * chunk, chunk)
        post_copies[i].wait()
        total = jnp.dot(post[0, rows, :], weights[0], preferred_element_type=F32)
        for k in range(1, anchors):
            total = total + jnp.dot(post[k, rows, :], weights[k], preferred_element_type=F32)
        high = total.astype(BF16)
        parts[rows, pl.ds(0, LANES)] = high
        parts[rows, pl.ds(LANES, LANES)] = (total - high.astype(F32)).astype(BF16)

    pl.semaphore_wait(barrier, chips - 1 + group - 1)

    kept = pl.ds(pl.multiple_of(core * rows_kept, 8), rows_kept)
    given = pl.ds(pl.multiple_of((1 - core) * rows_kept, 8), rows_kept)
    pair_copies = {}
    for step in order:
        both = jnp.dot(choose[step], parts[...], preferred_element_type=F32)
        sums = jnp.transpose(both[:, :LANES] + both[:, LANES:])
        for c in range(CORES):
            mine[step, pl.ds(c * rows_kept, rows_kept), :] = sums[c * HALF : c * HALF + rows_kept]
        copy = pltpu.make_async_remote_copy(
            src_ref=mine.at[step, given],
            dst_ref=pair_in.at[step],
            send_sem=pair_send.at[step],
            recv_sem=pair_recv.at[step],
            device_id={"hap": chip * CORES + 1 - core, "mk": mk},
            device_id_type=MESH,
        )
        copy.start()
        pair_copies[step] = copy

    chip_copies = {}
    for step in order:
        pair_copies[step].wait_recv()
        reduced[step] = mine[step, kept, :] + pair_in[step]
        if step:
            copy = pltpu.make_async_remote_copy(
                src_ref=reduced.at[step],
                dst_ref=chip_in.at[step],
                send_sem=chip_send.at[step],
                recv_sem=chip_recv.at[step],
                device_id=chip_peer(step),
                device_id_type=MESH,
            )
            copy.start()
            chip_copies[step] = copy

    total = reduced[0]
    for step in reversed(order[:-1]):
        chip_copies[step].wait_recv()
        total = total + chip_in[step]

    weight = (lax.broadcasted_iota(jnp.int32, (span, per_chip), 0).astype(F32) + 0.5) / span
    for l in range(local):
        base = 2 * l * span
        left = total[base : base + span] / total[body + l : body + l + 1]
        right = total[base + span : base + 2 * span] / total[body + l + 1 : body + l + 2]
        final[place, pl.ds(l * span, span), :] = (1.0 - weight) * left + weight * right

    final_copies = {}
    for step in range(1, group):
        copy = pltpu.make_async_remote_copy(
            src_ref=final.at[place],
            dst_ref=final.at[place],
            send_sem=final_send.at[step],
            recv_sem=final_recv.at[step],
            device_id=group_peer(step),
            device_id_type=MESH,
        )
        copy.start()
        final_copies[step] = copy
    for step in range(1, group):
        source = (place + group - step) % group
        pltpu.make_async_remote_copy(
            src_ref=final.at[source],
            dst_ref=final.at[source],
            send_sem=final_send.at[step],
            recv_sem=final_recv.at[step],
            device_id=group_peer(step),
            device_id_type=MESH,
        ).wait_recv()

    all_markers = final[...].reshape(group * local * span, per_chip)
    turned[...] = jnp.transpose(all_markers)
    out_ref[...] = own_rows(turned, core * mk_count + mk, per_device)

    for step in order:
        pair_copies[step].wait_send()
        if step:
            chip_copies[step].wait_send()
    for step in range(1, group):
        final_copies[step].wait_send()


def solution(mesh):
    hap_count, mk_count = mesh.shape["hap"], mesh.shape["mk"]
    steps = 4

    def on_device(posterior, alleles, owner_map):
        anchors, targets, refs = posterior.shape
        block = alleles.shape[1]
        intervals = anchors - 1
        local = intervals // CORES
        span = block // intervals
        chips = hap_count // CORES
        per_chip = targets // chips
        per_device = targets // (hap_count * mk_count)
        group = CORES * mk_count
        rows_kept = -(-(2 * local * span + local + 1) // 8) * 8
        scratch = [
            pltpu.VMEM(posterior.shape, BF16),
            pltpu.VMEM((block, refs), jnp.int32),
            pltpu.VMEM((1, targets), jnp.int32),
            pltpu.VMEM((anchors, refs, LANES), BF16),
            pltpu.VMEM((chips, per_chip, targets), BF16),
            pltpu.VMEM((targets, 2 * LANES), BF16),
            pltpu.VMEM((chips, CORES * rows_kept, per_chip), F32),
            pltpu.VMEM((chips, rows_kept, per_chip), F32),
            pltpu.VMEM((chips, rows_kept, per_chip), F32),
            pltpu.VMEM((chips, rows_kept, per_chip), F32),
            pltpu.VMEM((group, local * span, per_chip), F32),
            pltpu.VMEM((per_chip, mk_count * block), F32),
            pltpu.SemaphoreType.DMA((steps,)),
            pltpu.SemaphoreType.DMA((2,)),
        ] + [pltpu.SemaphoreType.DMA((chips,))] * 4 + [pltpu.SemaphoreType.DMA((group,))] * 2
        return pl.pallas_call(
            functools.partial(kernel, hap_count, mk_count, steps),
            out_shape=jax.ShapeDtypeStruct((per_device, mk_count * block), F32),
            in_specs=[pl.BlockSpec(memory_space=pltpu.HBM)] * 3,
            out_specs=pl.BlockSpec(memory_space=pltpu.VMEM),
            scratch_shapes=scratch,
            compiler_params=pltpu.CompilerParams(
                collective_id=0, has_side_effects=True, vmem_limit_bytes=48 * 1024 * 1024
            ),
        )(posterior, alleles.T, owner_map.reshape(1, targets))

    placed = (P("mk", None, "hap"), P("hap", "mk"), P())
    return jax.shard_map(
        on_device, mesh=mesh, in_specs=placed, out_specs=P(("hap", "mk"), None), check_vma=False
    )
```

```python
import functools

import jax
import jax.numpy as jnp
from jax import lax
from jax.experimental import pallas as pl
from jax.experimental.pallas import tpu as pltpu
from jax.sharding import PartitionSpec as P

LANES = 128
HALF = LANES // 2
CORES = 2
MESH = pl.DeviceIdType.MESH
F32 = jnp.float32
BF16 = jnp.bfloat16


def own_rows(ref, index, count):
    if count % 8 == 0:
        return ref[pl.ds(pl.multiple_of(index * count, 8), count), :]
    pieces = 8 // count
    tile = ref[pl.ds(pl.multiple_of((index // pieces) * 8, 8), 8), :]
    rows = tile[:count]
    for piece in range(1, pieces):
        rows = jnp.where(index % pieces == piece, tile[piece * count : (piece + 1) * count], rows)
    return rows


def kernel(
    hap_count,
    mk_count,
    steps,
    post_hbm,
    allele_hbm,
    owner_hbm,
    out_ref,
    post,
    allele,
    owner,
    weights,
    choose,
    parts,
    mine,
    pair_in,
    reduced,
    chip_in,
    final,
    turned,
    post_sem,
    small_sem,
    pair_send,
    pair_recv,
    chip_send,
    chip_recv,
    final_send,
    final_recv,
):
    anchors, targets, _ = post.shape
    block = allele.shape[0]
    intervals = anchors - 1
    span = block // intervals
    local = intervals // CORES
    body = 2 * local * span
    rows_kept = mine.shape[1] // CORES
    chips = hap_count // CORES
    per_chip = targets // chips
    devices = hap_count * mk_count
    per_device = targets // devices
    group = CORES * mk_count
    chunk = targets // steps

    hap, mk = lax.axis_index("hap"), lax.axis_index("mk")
    chip, core = hap // CORES, hap % CORES
    place = mk * CORES + core

    def chip_peer(step):
        return {"hap": ((chip + step) % chips) * CORES + core, "mk": mk}

    def group_peer(step):
        other = (place + step) % group
        return {"hap": chip * CORES + other % CORES, "mk": other // CORES}

    allele_copy = pltpu.make_async_copy(allele_hbm, allele, small_sem.at[0])
    owner_copy = pltpu.make_async_copy(owner_hbm, owner, small_sem.at[1])
    allele_copy.start()
    post_copies = []
    for i in range(steps):
        rows = pl.ds(i * chunk, chunk)
        copy = pltpu.make_async_copy(post_hbm.at[:, rows, :], post.at[:, rows, :], post_sem.at[i])
        copy.start()
        post_copies.append(copy)
        if i == 0:
            owner_copy.start()

    barrier = pltpu.get_barrier_semaphore()
    for step in range(1, chips):
        pl.semaphore_signal(barrier, inc=1, device_id=chip_peer(step), device_id_type=MESH)
    for step in range(1, group):
        pl.semaphore_signal(barrier, inc=1, device_id=group_peer(step), device_id_type=MESH)

    order = sorted(range(1, chips), key=lambda s: abs(s - chips // 2 - 0.5)) + [0]

    allele_copy.wait()
    col = lax.broadcasted_iota(jnp.int32, (block, LANES), 1)
    marker = lax.broadcasted_iota(jnp.int32, (block, LANES), 0)
    lane = lax.broadcasted_iota(jnp.int32, (1, LANES), 1)
    spread = jnp.zeros((block, LANES), F32)
    starts = []
    for j in range(intervals):
        for side in range(2):
            start = (j // local) * HALF + (j % local) * 2 * span + side * span
            starts.append((j + side, start))
            hit = (col - start == marker - j * span) & (col >= start) & (col < start + span)
            spread = spread + hit.astype(F32)
    wide = lax.dot_general(
        allele[...].astype(F32).astype(BF16),
        spread.astype(BF16),
        (((0,), (0,)), ((), ())),
        preferred_element_type=F32,
    )
    for k in range(anchors):
        inside = jnp.zeros((1, LANES), F32)
        for anchor, start in starts:
            if anchor == k:
                inside = inside + ((lane >= start) & (lane < start + span)).astype(F32)
        ones = jnp.zeros((1, LANES), F32)
        for c in range(CORES):
            if c * local <= k <= (c + 1) * local:
                ones = ones + (lane == c * HALF + body + k - c * local).astype(F32)
        weights[k] = (wide * inside + ones).astype(BF16)

    for i in range(steps):
        rows = pl.ds(i * chunk, chunk)
        post_copies[i].wait()
        if i == 0:
            owner_copy.wait()
            owners = owner[...]
            table = (lax.broadcasted_iota(jnp.int32, (devices, targets), 0) == owners).astype(F32)
            before = (
                lax.broadcasted_iota(jnp.int32, (LANES, LANES), 0)
                < lax.broadcasted_iota(jnp.int32, (LANES, LANES), 1)
            ).astype(F32).astype(BF16)
            carry = jnp.zeros((devices, 1), F32)
            ranks = []
            for b in range(targets // LANES):
                piece = table[:, b * LANES : (b + 1) * LANES]
                count = jnp.dot(piece.astype(BF16), before, preferred_element_type=F32) + carry
                ranks.append(jnp.sum(piece * count, axis=0, keepdims=True))
                carry = carry + jnp.sum(piece, axis=1, keepdims=True)
            row_of = owners.astype(F32) * per_device + jnp.concatenate(ranks, axis=1)
        for step in order[i::steps]:
            first = ((chip + step) % chips) * per_chip
            wanted = (lax.broadcasted_iota(jnp.int32, (per_chip, targets), 0) + first).astype(F32)
            choose[step] = (wanted == row_of).astype(F32).astype(BF16)
        total = jnp.dot(post[0, rows, :], weights[0], preferred_element_type=F32)
        for k in range(1, anchors):
            total = total + jnp.dot(post[k, rows, :], weights[k], preferred_element_type=F32)
        high = total.astype(BF16)
        parts[rows, pl.ds(0, LANES)] = high
        parts[rows, pl.ds(LANES, LANES)] = (total - high.astype(F32)).astype(BF16)

    pl.semaphore_wait(barrier, chips - 1 + group - 1)

    kept = pl.ds(pl.multiple_of(core * rows_kept, 8), rows_kept)
    given = pl.ds(pl.multiple_of((1 - core) * rows_kept, 8), rows_kept)
    pair_copies = {}
    chip_copies = {}
    lag = 3

    def pass_on(step):
        pair_copies[step].wait_recv()
        reduced[step] = mine[step, kept, :] + pair_in[step]
        if step:
            copy = pltpu.make_async_remote_copy(
                src_ref=reduced.at[step],
                dst_ref=chip_in.at[step],
                send_sem=chip_send.at[step],
                recv_sem=chip_recv.at[step],
                device_id=chip_peer(step),
                device_id_type=MESH,
            )
            copy.start()
            chip_copies[step] = copy

    for at, step in enumerate(order):
        both = jnp.dot(choose[step], parts[...], preferred_element_type=F32)
        sums = jnp.transpose(both[:, :LANES] + both[:, LANES:])
        for c in range(CORES):
            mine[step, pl.ds(c * rows_kept, rows_kept), :] = sums[c * HALF : c * HALF + rows_kept]
        copy = pltpu.make_async_remote_copy(
            src_ref=mine.at[step, given],
            dst_ref=pair_in.at[step],
            send_sem=pair_send.at[step],
            recv_sem=pair_recv.at[step],
            device_id={"hap": chip * CORES + 1 - core, "mk": mk},
            device_id_type=MESH,
        )
        copy.start()
        pair_copies[step] = copy
        if at >= lag:
            pass_on(order[at - lag])

    for step in order[-lag:]:
        pass_on(step)

    total = reduced[0]
    for step in reversed(order[:-1]):
        chip_copies[step].wait_recv()
        total = total + chip_in[step]

    weight = (lax.broadcasted_iota(jnp.int32, (span, per_chip), 0).astype(F32) + 0.5) / span
    for l in range(local):
        base = 2 * l * span
        left = total[base : base + span] / total[body + l : body + l + 1]
        right = total[base + span : base + 2 * span] / total[body + l + 1 : body + l + 2]
        final[place, pl.ds(l * span, span), :] = (1.0 - weight) * left + weight * right

    final_copies = {}
    for step in range(1, group):
        copy = pltpu.make_async_remote_copy(
            src_ref=final.at[place],
            dst_ref=final.at[place],
            send_sem=final_send.at[step],
            recv_sem=final_recv.at[step],
            device_id=group_peer(step),
            device_id_type=MESH,
        )
        copy.start()
        final_copies[step] = copy
    for step in range(1, group):
        source = (place + group - step) % group
        pltpu.make_async_remote_copy(
            src_ref=final.at[source],
            dst_ref=final.at[source],
            send_sem=final_send.at[step],
            recv_sem=final_recv.at[step],
            device_id=group_peer(step),
            device_id_type=MESH,
        ).wait_recv()

    all_markers = final[...].reshape(group * local * span, per_chip)
    turned[...] = jnp.transpose(all_markers)
    out_ref[...] = own_rows(turned, core * mk_count + mk, per_device)

    for step in order:
        pair_copies[step].wait_send()
        if step:
            chip_copies[step].wait_send()
    for step in range(1, group):
        final_copies[step].wait_send()


def solution(mesh):
    hap_count, mk_count = mesh.shape["hap"], mesh.shape["mk"]
    steps = 4

    def on_device(posterior, alleles, owner_map):
        anchors, targets, refs = posterior.shape
        block = alleles.shape[1]
        intervals = anchors - 1
        local = intervals // CORES
        span = block // intervals
        chips = hap_count // CORES
        per_chip = targets // chips
        per_device = targets // (hap_count * mk_count)
        group = CORES * mk_count
        rows_kept = -(-(2 * local * span + local + 1) // 8) * 8
        scratch = [
            pltpu.VMEM(posterior.shape, BF16),
            pltpu.VMEM((block, refs), jnp.int32),
            pltpu.VMEM((1, targets), jnp.int32),
            pltpu.VMEM((anchors, refs, LANES), BF16),
            pltpu.VMEM((chips, per_chip, targets), BF16),
            pltpu.VMEM((targets, 2 * LANES), BF16),
            pltpu.VMEM((chips, CORES * rows_kept, per_chip), F32),
            pltpu.VMEM((chips, rows_kept, per_chip), F32),
            pltpu.VMEM((chips, rows_kept, per_chip), F32),
            pltpu.VMEM((chips, rows_kept, per_chip), F32),
            pltpu.VMEM((group, local * span, per_chip), F32),
            pltpu.VMEM((per_chip, mk_count * block), F32),
            pltpu.SemaphoreType.DMA((steps,)),
            pltpu.SemaphoreType.DMA((2,)),
        ] + [pltpu.SemaphoreType.DMA((chips,))] * 4 + [pltpu.SemaphoreType.DMA((group,))] * 2
        return pl.pallas_call(
            functools.partial(kernel, hap_count, mk_count, steps),
            out_shape=jax.ShapeDtypeStruct((per_device, mk_count * block), F32),
            in_specs=[pl.BlockSpec(memory_space=pltpu.HBM)] * 3,
            out_specs=pl.BlockSpec(memory_space=pltpu.VMEM),
            scratch_shapes=scratch,
            compiler_params=pltpu.CompilerParams(
                collective_id=0, has_side_effects=True, vmem_limit_bytes=48 * 1024 * 1024
            ),
        )(posterior, alleles.T, owner_map.reshape(1, targets))

    placed = (P("mk", None, "hap"), P("hap", "mk"), P())
    return jax.shard_map(
        on_device, mesh=mesh, in_specs=placed, out_specs=P(("hap", "mk"), None), check_vma=False
    )
```
